256 devices in a mesh: grp: 8 (over z), sp: 32 (over y, x, core).
Axes of the slice: x: 4, y: 4, z: 8, core: 2. Of those that a mesh axis runs over, the one named last changes fastest.
Arguments:
- tokens: bfloat16 [16384, 2880], P(('grp', 'sp')), may hold values from -36 to 36
- query_weight: bfloat16 [2880, 2048], P(None, 'sp'), may hold values from -0.109375 to 0.109375
- key_value_weight: bfloat16 [2880, 1024], replicated, may hold values from -0.109375 to 0.109375
- block_places: int32 [32], replicated, may hold values from 0 to 31, each once
- sinks: float32 [32], replicated, may hold values from -1 to 5
Outputs:
- attended: bfloat16 [16384, 2048], P(('grp', 'sp'))
The draws below stay inside these ranges and needn't reach their ends.
Inputs may be any that keep to these rules, and one draw needn't show every extreme that they name: `block_places`: every sequence block appears once.
All inputs are finite; a program needn't handle non-finite values.
Results may differ from the reference program's by a relative error of at most 0.008.
The reference program's roundings to bfloat16 on the way count: a program that leaves them out, or rounds other values in their place, can miss the bound.
Values may be sent and summed in bfloat16 or wider, within the bound.
No kernel may reach another device: no remote copies, remote signals or barrier semaphores. Data moves between devices by JAX's collectives and lax.ppermute only.
A program may use at most 128 MiB of HBM per device.

```python
import jax
import jax.numpy as jnp
from jax import lax

MODEL_WIDTH = 2880
QUERY_HEADS = 32
KEY_VALUE_HEADS = 8
HEAD_SIZE = 64
BLK = 512
NBLK = 32
SEQUENCE_TOKENS = 16384


def draw_tokens(key, part):
    base = jnp.clip(jax.random.normal(key, (SEQUENCE_TOKENS, MODEL_WIDTH), jnp.float32), -6.0, 6.0)
    return base.astype(jnp.bfloat16)


def block_levels(stream_key, extent, split, smallest, high):
    def one(position, shards_of):
        draws = jax.random.uniform(jax.random.fold_in(jax.random.fold_in(stream_key, 6), position), (shards_of,), jnp.float32, smallest / len(split), high / len(split))
        return jnp.repeat(jnp.exp(draws), extent[position] // shards_of).reshape((-1,) + (1,) * (len(extent) - position - 1))

    loudness = one(*split[0])
    for cut in split[1:]:
        loudness = loudness * one(*cut)
    return loudness


def scatter_about(stream_key, extent, width, most, cuts=(), kind=jnp.bfloat16):
    level = block_levels(stream_key, extent, cuts, -0.22, 0.18) if cuts else 1.0
    entries = jax.random.normal(stream_key, extent, jnp.float32) * width * level
    return jnp.minimum(jnp.maximum(entries, -most), most).astype(kind)


def setup_inputs(seed: int = 0) -> dict:
    keys = jax.random.split(jax.random.key(seed), 6)
    tokens = draw_tokens(jax.random.fold_in(keys[5], 71), 0)
    query_weight = scatter_about(keys[1], (MODEL_WIDTH, QUERY_HEADS * HEAD_SIZE), MODEL_WIDTH ** -0.5, 0.109375, ((1, 32),))
    key_value_weight = scatter_about(keys[2], (MODEL_WIDTH, 2 * KEY_VALUE_HEADS * HEAD_SIZE), MODEL_WIDTH ** -0.5, 0.109375)
    block_places = jax.random.permutation(keys[3], NBLK).astype(jnp.int32)
    sinks = jnp.clip(jax.random.uniform(keys[4], (QUERY_HEADS,), jnp.float32, -1.0, 5.0), -1.0, 5.0)
    return {"tokens": tokens, "query_weight": query_weight, "key_value_weight": key_value_weight, "block_places": block_places, "sinks": sinks}


rope_base = 150000.0
neg_large = -1.0e30


def rotate(vectors, angles):
    middle = vectors.shape[-1] // 2
    first_half = vectors[..., :middle]
    second_half = vectors[..., middle:]
    cosine = jnp.cos(angles)
    sine_part = jnp.sin(angles)
    return jnp.concatenate([first_half * cosine - second_half * sine_part, second_half * cosine + first_half * sine_part], axis=-1)


def reference(tokens, query_weight, key_value_weight, block_places, sinks):
    stored = jnp.arange(SEQUENCE_TOKENS, dtype=jnp.int32)
    blocks = stored // BLK
    places = block_places[blocks] * BLK + stored % BLK
    inverse = rope_base ** (-(jnp.arange(HEAD_SIZE // 2, dtype=jnp.float32) * 2.0) / HEAD_SIZE)
    angles = places.astype(jnp.float32)[:, None, None] * inverse[None, None, :]
    queries = jnp.dot(tokens, query_weight, preferred_element_type=jnp.float32).reshape(SEQUENCE_TOKENS, QUERY_HEADS, HEAD_SIZE)
    key_value_pair = jnp.dot(tokens, key_value_weight, preferred_element_type=jnp.float32)
    key_head_rows = key_value_pair[:, :KEY_VALUE_HEADS * HEAD_SIZE].reshape(SEQUENCE_TOKENS, KEY_VALUE_HEADS, HEAD_SIZE)
    value_head_rows = key_value_pair[:, KEY_VALUE_HEADS * HEAD_SIZE:].reshape(SEQUENCE_TOKENS, KEY_VALUE_HEADS, HEAD_SIZE).astype(jnp.bfloat16)
    queries = rotate(queries, angles).astype(jnp.bfloat16)
    key_head_rows = rotate(key_head_rows, angles).astype(jnp.bfloat16)
    query_sharing = QUERY_HEADS // KEY_VALUE_HEADS
    score_scale = HEAD_SIZE ** -0.5

    def single_head(head_number):
        head_keys = lax.dynamic_index_in_dim(key_head_rows, head_number, 1, keepdims=False).astype(jnp.float32)
        head_values = lax.dynamic_index_in_dim(value_head_rows, head_number, 1, keepdims=False).astype(jnp.float32)
        head_queries = lax.dynamic_slice_in_dim(queries, head_number * query_sharing, query_sharing, 1)
        head_sinks = lax.dynamic_slice_in_dim(sinks, head_number * query_sharing, query_sharing, 0)

        def one_block(query_block):
            first_row = query_block * BLK
            query_rows = lax.dynamic_slice_in_dim(head_queries, first_row, BLK, 0).astype(jnp.float32)
            row_places = lax.dynamic_slice_in_dim(places, first_row, BLK, 0)
            scores = jnp.einsum("qgd,kd->gqk", query_rows, head_keys) * score_scale
            allowed = places[None, :] <= row_places[:, None]
            scores = jnp.where(allowed[None], scores, neg_large)
            highest = jnp.maximum(jnp.max(scores, axis=-1, keepdims=True), head_sinks[:, None, None])
            weights = jnp.where(allowed[None], jnp.exp(scores - highest), 0.0)
            totals = jnp.sum(weights, axis=-1) + jnp.exp(head_sinks[:, None] - highest[..., 0])
            rounded = lax.optimization_barrier(weights.astype(jnp.bfloat16)).astype(jnp.float32)
            mixture = jnp.einsum("gqk,kd->qgd", rounded, head_values)
            return mixture / jnp.transpose(totals)[:, :, None]

        return lax.map(one_block, jnp.arange(SEQUENCE_TOKENS // BLK, dtype=jnp.int32))

    layer_output = lax.map(single_head, jnp.arange(KEY_VALUE_HEADS, dtype=jnp.int32))
    layer_output = jnp.transpose(layer_output, (1, 2, 0, 3, 4)).reshape(SEQUENCE_TOKENS, QUERY_HEADS * HEAD_SIZE)
    return layer_output.astype(jnp.bfloat16)
```

```python
import jax
import jax.numpy as jnp
from jax import lax
from jax.experimental import pallas as pl
from jax.experimental.pallas import tpu as pltpu
from jax.sharding import Mesh, PartitionSpec as P

HEAD = 64
NBLK = 32
BLK = 512
ROWS = 64
ROPE_BASE = 150000.0
NEG = -1e30
EXPC = 1.4426950408889634 / 8.0
BF = jnp.bfloat16
F32 = jnp.float32


def attend_kernel(inv_ref, meta_ref, sink_ref, kv_ref, q_ref, o_ref, kvs, vts, qs, s_scr, cm_scr):
    off = meta_ref[0]
    y_own = meta_ref[1]
    c_own = meta_ref[2]

    @pl.loop(0, NBLK)
    def _(s):
        b = inv_ref[s]
        z = b // 4
        piece = lax.rem(lax.rem(b, 4) - y_own + 4, 4)
        for o in range(8):
            core = o % 2 - c_own
            kvs[pl.ds(pl.multiple_of(s * BLK + o * ROWS, ROWS), ROWS), :] = kv_ref[
                z, o // 2, core * core, piece
            ]
        t = jnp.transpose(kvs[pl.ds(pl.multiple_of(s * BLK, BLK), BLK), :])
        vts[s, 0:HEAD, :] = t[HEAD : 2 * HEAD, :]
        vts[s, HEAD : HEAD + 16, :] = jnp.ones((16, BLK), BF)

    for k in range(8):
        rows = jnp.transpose(q_ref[k])
        wide = jnp.concatenate([rows, jnp.zeros((4 * ROWS, HEAD), BF)], axis=1)
        qs[k] = wide.reshape(4, ROWS, 2 * HEAD)

    def qtile(i):
        parts = []
        for j in range(4):
            b = inv_ref[i * 4 + j]
            parts.append(qs[b // 4, lax.rem(lax.rem(b, 4) - y_own + 4, 4)])
        return jnp.concatenate(parts, axis=0)

    def qk(i, s, slot, diag):
        keys = kvs[pl.ds(pl.multiple_of(s * BLK, BLK), BLK), :]
        scores = lax.dot_general(
            keys, qtile(i), (((1,), (1,)), ((), ())), preferred_element_type=F32
        )
        if diag is not None:
            row = lax.broadcasted_iota(jnp.int32, (BLK, 256), 0) + diag * BLK
            col = lax.broadcasted_iota(jnp.int32, (1, 256), 1)
            limit = (col // ROWS) * BLK + lax.rem(col, ROWS) + off
            scores = jnp.where(row <= limit, scores, NEG)
        s_scr[slot] = scores
        cm_scr[slot] = jnp.max(scores.reshape(BLK // 8, 8, 256), axis=0)

    def soft(s, slot, m, acc):
        new = jnp.maximum(m, jnp.max(cm_scr[slot], axis=0, keepdims=True))
        factor = jnp.exp2((m - new) * EXPC)
        weight = jnp.exp2((s_scr[slot] - new) * EXPC).astype(BF)
        return new, acc * factor + jnp.dot(vts[s], weight, preferred_element_type=F32)

    def tile(i, _):
        m = jnp.full((1, 256), sink_ref[0] * 8.0, F32)
        acc = jnp.concatenate([jnp.zeros((HEAD, 256), F32), jnp.ones((16, 256), F32)], axis=0)

        def full(j, carry):
            m, acc = carry
            for u in range(4):
                if u < 3:
                    qk(i, j * 4 + u + 1, (u + 1) % 2, None)
                else:

                    @pl.when(j + 1 < i)
                    def _():
                        qk(i, j * 4 + 4, 0, None)

                    @pl.when(j + 1 == i)
                    def _():
                        qk(i, j * 4 + 4, 0, 0)

                m, acc = soft(j * 4 + u, u % 2, m, acc)
            return m, acc

        m, acc = lax.fori_loop(0, i, full, (m, acc))
        for u in range(4):
            if u < 3:
                qk(i, i * 4 + u + 1, (u + 1) % 2, u + 1)
            else:
                qk(jnp.minimum(i + 1, 7), 0, 0, None)
            m, acc = soft(i * 4 + u, u % 2, m, acc)
        done = jnp.transpose(acc[0:HEAD] / acc[HEAD : HEAD + 1]).astype(BF)
        for j in range(4):
            rows = done[j * ROWS : (j + 1) * ROWS]
            o_ref[inv_ref[i * 4 + j]] = jnp.concatenate([rows[0:32], rows[32:64]], axis=1)
        return 0

    qk(0, 0, 0, 0)
    lax.fori_loop(0, 8, tile, 0)


def attend(inv, meta, sink, kv, q):
    return pl.pallas_call(
        attend_kernel,
        out_shape=jax.ShapeDtypeStruct((NBLK, 32, 128), BF),
        in_specs=[pl.BlockSpec(memory_space=pltpu.SMEM)] * 3
        + [pl.BlockSpec(memory_space=pltpu.VMEM)] * 2,
        out_specs=pl.BlockSpec(memory_space=pltpu.VMEM),
        scratch_shapes=[
            pltpu.VMEM((NBLK * BLK, 2 * HEAD), BF),
            pltpu.VMEM((NBLK, HEAD + 16, BLK), BF),
            pltpu.VMEM((8, 4, ROWS, 2 * HEAD), BF),
            pltpu.VMEM((2, BLK, 256), F32),
            pltpu.VMEM((2, 8, 256), F32),
        ],
        compiler_params=pltpu.CompilerParams(vmem_limit_bytes=50 * 2**20),
        name="attend",
    )(inv, meta, sink, kv, q)


def pull(value, axis, shift):
    size = lax.axis_size(axis)
    return lax.ppermute(value, axis, [((i + shift) % size, i) for i in range(size)])


def swap(value):
    return lax.ppermute(value, "c", [(0, 1), (1, 0)])


def pick(array, index):
    return lax.dynamic_index_in_dim(array, index, 0, keepdims=False)


def ordered(own, other, c):
    return lax.dynamic_slice_in_dim(jnp.stack([own, other, own]), c, 2, 0)


def per_device(tokens, query_weight, key_value_weight, block_places, sinks):
    z, y, x, c = (lax.axis_index(a) for a in "zyxc")
    weight_rows = query_weight.T
    rows = jnp.concatenate([tokens] + [pull(tokens, "y", s) for s in (1, 2, 3)], axis=0)
    weights = jnp.concatenate([weight_rows] + [pull(weight_rows, "x", s) for s in (1, 2, 3)], axis=0)
    weights_other = swap(weights)

    table = jnp.arange(NBLK, dtype=jnp.int32)
    block_of = jnp.sum(
        jnp.where(block_places[None, :] == table[:, None], table[None, :], 0), axis=1
    ).astype(jnp.int32)
    own_blocks = 4 * z + (y + jnp.arange(4, dtype=jnp.int32)) % 4
    own_places = jnp.sum(
        jnp.where(own_blocks[:, None] == table[None, :], block_places[None, :], 0), axis=1
    )
    places = (
        own_places[:, None] * BLK + (2 * x + c) * ROWS + jnp.arange(ROWS, dtype=jnp.int32)[None, :]
    ).reshape(4 * ROWS)
    inverse = ROPE_BASE ** (-(jnp.arange(HEAD // 2, dtype=F32) * 2.0) / HEAD)
    angles = places.astype(F32)[None, :] * inverse[:, None]
    cos, sin = jnp.cos(angles), jnp.sin(angles)

    key_weight = lax.dynamic_slice_in_dim(key_value_weight, 128 * y, 128, 1)
    value_weight = lax.dynamic_slice_in_dim(key_value_weight, 512 + 128 * y, 128, 1)
    kv = jnp.dot(
        rows, jnp.concatenate([key_weight, value_weight], axis=1), preferred_element_type=F32
    )
    first, second = (kv[:, :128].reshape(4 * ROWS, 2, 2, 32)[:, :, h] for h in (0, 1))
    cos_rows, sin_rows = cos.T[:, None, :], sin.T[:, None, :]
    keys = jnp.concatenate(
        [first * cos_rows - second * sin_rows, second * cos_rows + first * sin_rows], axis=-1
    )
    pair = jnp.concatenate([keys, kv[:, 128:].reshape(4 * ROWS, 2, HEAD)], axis=-1).astype(BF)
    pair = jnp.transpose(pair, (1, 0, 2))
    both = jnp.stack([pick(pair, c), swap(pick(pair, 1 - c))])
    kv_all = lax.all_gather(both, ("z", "x"), axis=0, tiled=False)
    kv_all = kv_all.reshape(8, 4, 2, 4, ROWS, 2 * HEAD)

    def project(w):
        q = lax.dot_general(w, rows, (((1,), (1,)), ((), ())), preferred_element_type=F32)
        q = q.reshape(4, 2, 32, 4 * ROWS)
        a, b = q[:, 0], q[:, 1]
        return jnp.concatenate([a * cos - b * sin, b * cos + a * sin], axis=1).astype(BF)

    q = ordered(project(weights), project(weights_other), c)
    q = lax.dynamic_slice_in_dim(jnp.concatenate([q, q], axis=1), (4 - x) % 4, 4, 1)
    q = jnp.transpose(q.reshape(2, 2, 2, HEAD, 4 * ROWS), (1, 2, 0, 3, 4))
    q = q.reshape(2, 4, HEAD, 4 * ROWS)
    q = ordered(pick(q, c), swap(pick(q, 1 - c)), c)
    q = lax.all_to_all(q.reshape(8, HEAD, 4 * ROWS), "z", 0, 0, tiled=True)

    slot = jnp.arange(3, dtype=jnp.int32)
    meta = jnp.where(slot == 0, ROWS * (2 * x + z // 4), jnp.where(slot == 1, y, c))
    sink = lax.dynamic_slice_in_dim(sinks, 8 * y + 4 * c + z % 4, 1, 0)
    out = attend(block_of, meta.astype(jnp.int32), sink, kv_all, q)

    out = lax.all_to_all(out, ("z", "y"), 0, 0, tiled=True)
    out = out.reshape(2, 4, 4, 32, 128)
    out = ordered(pick(out, c), swap(pick(out, 1 - c)), c)
    out = out.reshape(2, 4, 4, 32, 2, HEAD)
    return jnp.transpose(out, (4, 3, 2, 0, 1, 5)).reshape(ROWS, 32 * HEAD)


def solution(mesh):
    fine = Mesh(mesh.devices.reshape(8, 4, 4, 2), ("z", "y", "x", "c"))
    whole = ("z", "y", "x", "c")
    return jax.shard_map(
        per_device,
        mesh=fine,
        in_specs=(P(whole, None), P(None, ("y", "x", "c")), P(), P(), P()),
        out_specs=P(whole, None),
        check_vma=False,
    )
```

```python
import jax
import jax.numpy as jnp
from jax import lax
from jax.experimental import pallas as pl
from jax.experimental.pallas import tpu as pltpu
from jax.sharding import Mesh, PartitionSpec as P


HEAD = 64
NBLK = 32
BLK = 512
ROWS = 64
ROPE_BASE = 150000.0
NEG = -1e30
EXPC = 1.4426950408889634 / 8.0
BF = jnp.bfloat16
F32 = jnp.float32


def attend_kernel(
    inv_ref, meta_ref, sink_ref, own_ref, other_ref, q_ref, o_ref, kvs, vts, qs, s_scr, cm_scr
):
    off = meta_ref[0]
    y_tile = meta_ref[1]
    core = meta_ref[2]

    @pl.loop(0, NBLK)
    def _(s):
        b = inv_ref[s]
        for px in range(4):
            for ref, at in ((own_ref, core), (other_ref, 1 - core)):
                start = pl.multiple_of(s * BLK + (2 * px + at) * ROWS, ROWS)
                kvs[pl.ds(start, ROWS), :] = ref[lax.rem(b, 4), px, b // 4]
        t = jnp.transpose(kvs[pl.ds(pl.multiple_of(s * BLK, BLK), BLK), :])
        vts[s, 0:HEAD, :] = t[HEAD : 2 * HEAD, :]
        vts[s, HEAD : HEAD + 16, :] = jnp.ones((16, BLK), BF)

    for k in range(8):
        rows = jnp.transpose(q_ref[k])
        wide = jnp.concatenate([rows, jnp.zeros((4 * ROWS, HEAD), BF)], axis=1)
        qs[k] = wide.reshape(4, ROWS, 2 * HEAD)

    def qtile(i):
        parts = []
        for j in range(4):
            b = inv_ref[i * 4 + j]
            parts.append(qs[b // 4, lax.rem(lax.rem(b, 4) - y_tile + 4, 4)])
        return jnp.concatenate(parts, axis=0)

    def qk(i, s, slot, diag):
        keys = kvs[pl.ds(pl.multiple_of(s * BLK, BLK), BLK), :]
        scores = lax.dot_general(
            keys, qtile(i), (((1,), (1,)), ((), ())), preferred_element_type=F32
        )
        if diag is not None:
            row = lax.broadcasted_iota(jnp.int32, (BLK, 256), 0) + diag * BLK
            col = lax.broadcasted_iota(jnp.int32, (1, 256), 1)
            limit = (col // ROWS) * BLK + lax.rem(col, ROWS) + off
            scores = jnp.where(row <= limit, scores, NEG)
        s_scr[slot] = scores
        cm_scr[slot] = jnp.max(scores.reshape(BLK // 8, 8, 256), axis=0)

    def soft(s, slot, m, acc):
        new = jnp.maximum(m, jnp.max(cm_scr[slot], axis=0, keepdims=True))
        factor = jnp.exp2((m - new) * EXPC)
        weight = jnp.exp2((s_scr[slot] - new) * EXPC).astype(BF)
        return new, acc * factor + jnp.dot(vts[s], weight, preferred_element_type=F32)

    def tile(i, _):
        m = jnp.full((1, 256), sink_ref[0] * 8.0, F32)
        acc = jnp.concatenate([jnp.zeros((HEAD, 256), F32), jnp.ones((16, 256), F32)], axis=0)

        def full(j, carry):
            m, acc = carry
            for u in range(4):
                if u < 3:
                    qk(i, j * 4 + u + 1, (u + 1) % 2, None)
                else:

                    @pl.when(j + 1 < i)
                    def _():
                        qk(i, j * 4 + 4, 0, None)

                    @pl.when(j + 1 == i)
                    def _():
                        qk(i, j * 4 + 4, 0, 0)

                m, acc = soft(j * 4 + u, u % 2, m, acc)
            return m, acc

        m, acc = lax.fori_loop(0, i, full, (m, acc))
        for u in range(4):
            if u < 3:
                qk(i, i * 4 + u + 1, (u + 1) % 2, u + 1)
            else:
                qk(jnp.minimum(i + 1, 7), 0, 0, None)
            m, acc = soft(i * 4 + u, u % 2, m, acc)
        done = jnp.transpose(acc[0:HEAD] / acc[HEAD : HEAD + 1]).astype(BF)
        for j in range(4):
            rows = done[j * ROWS : (j + 1) * ROWS]
            o_ref[inv_ref[i * 4 + j]] = jnp.concatenate([rows[0:32], rows[32:64]], axis=1)
        return 0

    qk(0, 0, 0, 0)
    lax.fori_loop(0, 8, tile, 0)


def attend(inv, meta, sink, own, other, q):
    return pl.pallas_call(
        attend_kernel,
        out_shape=jax.ShapeDtypeStruct((NBLK, 32, 128), BF),
        in_specs=[pl.BlockSpec(memory_space=pltpu.SMEM)] * 3
        + [pl.BlockSpec(memory_space=pltpu.VMEM)] * 3,
        out_specs=pl.BlockSpec(memory_space=pltpu.VMEM),
        scratch_shapes=[
            pltpu.VMEM((NBLK * BLK, 2 * HEAD), BF),
            pltpu.VMEM((NBLK, HEAD + 16, BLK), BF),
            pltpu.VMEM((8, 4, ROWS, 2 * HEAD), BF),
            pltpu.VMEM((2, BLK, 256), F32),
            pltpu.VMEM((2, 8, 256), F32),
        ],
        compiler_params=pltpu.CompilerParams(vmem_limit_bytes=50 * 2**20),
        name="attend",
    )(inv, meta, sink, own, other, q)


def pull(value, axis, shift):
    size = lax.axis_size(axis)
    return lax.ppermute(value, axis, [((i + shift) % size, i) for i in range(size)])


def swap(value):
    return lax.ppermute(value, "c", [(0, 1), (1, 0)])


def ordered(own, other, c):
    return lax.dynamic_slice_in_dim(jnp.stack([own, other, own]), c, 2, 0)


def rotations(places):
    inverse = ROPE_BASE ** (-(jnp.arange(HEAD // 2, dtype=F32) * 2.0) / HEAD)
    angles = places.astype(F32)[None, :] * inverse[:, None]
    return jnp.cos(angles), jnp.sin(angles)


def per_device(tokens, query_weight, key_value_weight, block_places, sinks):
    z, y, x, c = (lax.axis_index(a) for a in "zyxc")
    weight_rows = query_weight.T
    row_pieces = [tokens] + [pull(tokens, "y", s) for s in (1, 2, 3)]
    weight_pieces = [weight_rows] + [pull(weight_rows, "x", s) for s in (1, 2, 3)]

    table = jnp.arange(NBLK, dtype=jnp.int32)
    block_of = jnp.sum(
        jnp.where(block_places[None, :] == table[:, None], table[None, :], 0), axis=1
    ).astype(jnp.int32)
    own_blocks = 4 * z + (y + jnp.arange(4, dtype=jnp.int32)) % 4
    own_places = jnp.sum(
        jnp.where(own_blocks[:, None] == table[None, :], block_places[None, :], 0), axis=1
    )
    places = (
        own_places[:, None] * BLK + (2 * x + c) * ROWS + jnp.arange(ROWS, dtype=jnp.int32)[None, :]
    )

    cos, sin = (t.T[:, None, :] for t in rotations(places[0]))
    kv = jnp.dot(tokens, key_value_weight, preferred_element_type=F32)
    keys = kv[:, :512].reshape(ROWS, 8, 2, 32)
    first, second = keys[:, :, 0], keys[:, :, 1]
    keys = jnp.concatenate([first * cos - second * sin, second * cos + first * sin], axis=-1)
    pair = jnp.concatenate([keys, kv[:, 512:].reshape(ROWS, 8, HEAD)], axis=-1).astype(BF)
    pair = lax.all_to_all(jnp.transpose(pair, (1, 0, 2)), "z", 0, 0, tiled=True)
    copies = jnp.broadcast_to(pair[None], (16, 8, ROWS, 2 * HEAD)).reshape(128, ROWS, 2 * HEAD)
    own = lax.all_to_all(copies, ("y", "x"), 0, 0, tiled=True)
    own = own.reshape(4, 4, 8, ROWS, 2 * HEAD)
    other = swap(own)

    rows = jnp.concatenate(row_pieces, axis=0)
    weights = jnp.concatenate(weight_pieces, axis=0)
    weights_other = swap(weights)
    cos_q, sin_q = rotations(places.reshape(4 * ROWS))

    def project(w):
        q = lax.dot_general(w, rows, (((1,), (1,)), ((), ())), preferred_element_type=F32)
        q = q.reshape(4, 2, 32, 4 * ROWS)
        a, b = q[:, 0], q[:, 1]
        return jnp.concatenate([a * cos_q - b * sin_q, b * cos_q + a * sin_q], axis=1).astype(BF)

    q = ordered(project(weights), project(weights_other), c)
    q = lax.dynamic_slice_in_dim(jnp.concatenate([q, q], axis=1), (4 - x) % 4, 4, 1)
    q = jnp.transpose(q.reshape(2, 2, 2, HEAD, 4 * ROWS), (2, 0, 1, 3, 4))
    q = lax.all_to_all(q.reshape(8, HEAD, 4 * ROWS), "y", 0, 0, tiled=True)
    q = lax.all_to_all(q, "z", 0, 0, tiled=True)

    slot = jnp.arange(3, dtype=jnp.int32)
    meta = jnp.where(slot == 0, ROWS * (2 * x + c), jnp.where(slot == 1, z // 2, c))
    sink = lax.dynamic_slice_in_dim(sinks, 4 * z + y, 1, 0)
    out = attend(block_of, meta.astype(jnp.int32), sink, own, other, q)

    out = lax.all_to_all(out, ("z", "y"), 0, 0, tiled=True)
    out = out.reshape(32, 32, 2, HEAD)
    return jnp.transpose(out, (2, 1, 0, 3)).reshape(ROWS, 32 * HEAD)


def solution(mesh):
    fine = Mesh(mesh.devices.reshape(8, 4, 4, 2), ("z", "y", "x", "c"))
    whole = ("z", "y", "x", "c")

    return jax.shard_map(
        per_device,
        mesh=fine,
        in_specs=(P(whole, None), P(None, ("y", "x", "c")), P(), P(), P()),
        out_specs=P(whole, None),
        check_vma=False,
    )
```

```python
import jax
import jax.numpy as jnp
from jax import lax
from jax.experimental import pallas as pl
from jax.experimental.pallas import tpu as pltpu
from jax.sharding import Mesh, PartitionSpec as P


HEAD = 64
NBLK = 32
BLK = 512
ROWS = 64
ROPE_BASE = 150000.0
NEG = -1e30
EXPC = 1.4426950408889634 / 8.0
BF = jnp.bfloat16
F32 = jnp.float32


def attend_kernel(
    inv_ref, meta_ref, sink_ref, k0, k1, k2, k3, o0, o1, o2, o3, q_ref, o_ref, kvs, vts, qs, s_scr, cm_scr
):
    x_own = meta_ref[0]
    y_tile = meta_ref[1]
    core = meta_ref[2]
    off = (2 * x_own + core) * ROWS

    @pl.loop(0, NBLK)
    def _(s):
        b = inv_ref[s]
        for step, pair in enumerate(((k0, o0), (k1, o1), (k2, o2), (k3, o3))):
            for ref, at in zip(pair, (core, 1 - core)):
                place = 2 * lax.rem(x_own + step, 4) + at
                start = pl.multiple_of(s * BLK + place * ROWS, ROWS)
                kvs[pl.ds(start, ROWS), :] = ref[b]
        t = jnp.transpose(kvs[pl.ds(pl.multiple_of(s * BLK, BLK), BLK), :])
        vts[s, 0:HEAD, :] = t[HEAD : 2 * HEAD, :]
        vts[s, HEAD : HEAD + 16, :] = jnp.ones((16, BLK), BF)

    for k in range(8):
        rows = jnp.transpose(q_ref[k])
        wide = jnp.concatenate([rows, jnp.zeros((4 * ROWS, HEAD), BF)], axis=1)
        qs[k] = wide.reshape(4, ROWS, 2 * HEAD)

    def qtile(i):
        parts = []
        for j in range(4):
            b = inv_ref[i * 4 + j]
            parts.append(qs[b // 4, lax.rem(lax.rem(b, 4) - y_tile + 4, 4)])
        return jnp.concatenate(parts, axis=0)

    def qk(i, s, slot, diag):
        keys = kvs[pl.ds(pl.multiple_of(s * BLK, BLK), BLK), :]
        scores = lax.dot_general(
            keys, qtile(i), (((1,), (1,)), ((), ())), preferred_element_type=F32
        )
        if diag is not None:
            row = lax.broadcasted_iota(jnp.int32, (BLK, 256), 0) + diag * BLK
            col = lax.broadcasted_iota(jnp.int32, (1, 256), 1)
            limit = (col // ROWS) * BLK + lax.rem(col, ROWS) + off
            scores = jnp.where(row <= limit, scores, NEG)
        s_scr[slot] = scores
        cm_scr[slot] = jnp.max(scores.reshape(BLK // 8, 8, 256), axis=0)

    def soft(s, slot, m, acc):
        new = jnp.maximum(m, jnp.max(cm_scr[slot], axis=0, keepdims=True))
        factor = jnp.exp2((m - new) * EXPC)
        weight = jnp.exp2((s_scr[slot] - new) * EXPC).astype(BF)
        return new, acc * factor + jnp.dot(vts[s], weight, preferred_element_type=F32)

    def tile(i, _):
        m = jnp.full((1, 256), sink_ref[0] * 8.0, F32)
        acc = jnp.concatenate([jnp.zeros((HEAD, 256), F32), jnp.ones((16, 256), F32)], axis=0)

        def full(j, carry):
            m, acc = carry
            for u in range(4):
                if u < 3:
                    qk(i, j * 4 + u + 1, (u + 1) % 2, None)
                else:

                    @pl.when(j + 1 < i)
                    def _():
                        qk(i, j * 4 + 4, 0, None)

                    @pl.when(j + 1 == i)
                    def _():
                        qk(i, j * 4 + 4, 0, 0)

                m, acc = soft(j * 4 + u, u % 2, m, acc)
            return m, acc

        m, acc = lax.fori_loop(0, i, full, (m, acc))
        for u in range(4):
            if u < 3:
                qk(i, i * 4 + u + 1, (u + 1) % 2, u + 1)
            else:
                qk(jnp.minimum(i + 1, 7), 0, 0, None)
            m, acc = soft(i * 4 + u, u % 2, m, acc)
        done = jnp.transpose(acc[0:HEAD] / acc[HEAD : HEAD + 1]).astype(BF)
        for j in range(4):
            rows = done[j * ROWS : (j + 1) * ROWS]
            o_ref[inv_ref[i * 4 + j]] = jnp.concatenate([rows[0:32], rows[32:64]], axis=1)
        return 0

    qk(0, 0, 0, 0)
    lax.fori_loop(0, 8, tile, 0)


def attend(inv, meta, sink, own, other, q):
    return pl.pallas_call(
        attend_kernel,
        out_shape=jax.ShapeDtypeStruct((NBLK, 32, 128), BF),
        in_specs=[pl.BlockSpec(memory_space=pltpu.SMEM)] * 3
        + [pl.BlockSpec(memory_space=pltpu.VMEM)] * 9,
        out_specs=pl.BlockSpec(memory_space=pltpu.VMEM),
        scratch_shapes=[
            pltpu.VMEM((NBLK * BLK, 2 * HEAD), BF),
            pltpu.VMEM((NBLK, HEAD + 16, BLK), BF),
            pltpu.VMEM((8, 4, ROWS, 2 * HEAD), BF),
            pltpu.VMEM((2, BLK, 256), F32),
            pltpu.VMEM((2, 8, 256), F32),
        ],
        compiler_params=pltpu.CompilerParams(vmem_limit_bytes=50 * 2**20),
        name="attend",
    )(inv, meta, sink, *own, *other, q)


def pull(value, axis, shift):
    size = lax.axis_size(axis)
    return lax.ppermute(value, axis, [((i + shift) % size, i) for i in range(size)])


def swap(value):
    return lax.ppermute(value, "c", [(0, 1), (1, 0)])


def ordered(own, other, c):
    return lax.dynamic_slice_in_dim(jnp.stack([own, other, own]), c, 2, 0)


def rotations(places):
    inverse = ROPE_BASE ** (-(jnp.arange(HEAD // 2, dtype=F32) * 2.0) / HEAD)
    angles = places.astype(F32)[None, :] * inverse[:, None]
    return jnp.cos(angles), jnp.sin(angles)


def per_device(tokens, query_weight, key_value_weight, block_places, sinks):
    z, y, x, c = (lax.axis_index(a) for a in "zyxc")
    weight_rows = query_weight.T
    row_pieces = [tokens] + [pull(tokens, "y", s) for s in (1, 2, 3)]
    weight_pieces = [weight_rows] + [pull(weight_rows, "x", s) for s in (1, 2, 3)]

    table = jnp.arange(NBLK, dtype=jnp.int32)
    block_of = jnp.sum(
        jnp.where(block_places[None, :] == table[:, None], table[None, :], 0), axis=1
    ).astype(jnp.int32)
    own_blocks = 4 * z + (y + jnp.arange(4, dtype=jnp.int32)) % 4
    own_places = jnp.sum(
        jnp.where(own_blocks[:, None] == table[None, :], block_places[None, :], 0), axis=1
    )
    places = (
        own_places[:, None] * BLK + (2 * x + c) * ROWS + jnp.arange(ROWS, dtype=jnp.int32)[None, :]
    )

    cos, sin = (t.T[:, None, :] for t in rotations(places[0]))
    kv = jnp.dot(tokens, key_value_weight, preferred_element_type=F32)
    keys = kv[:, :512].reshape(ROWS, 8, 2, 32)
    first, second = keys[:, :, 0], keys[:, :, 1]
    keys = jnp.concatenate([first * cos - second * sin, second * cos + first * sin], axis=-1)
    pair = jnp.concatenate([keys, kv[:, 512:].reshape(ROWS, 8, HEAD)], axis=-1).astype(BF)
    pair = jnp.transpose(pair.reshape(ROWS, 4, 2, 2 * HEAD), (2, 1, 0, 3))
    pair = jnp.broadcast_to(pair[:, None], (2, 4, 4, ROWS, 2 * HEAD)).reshape(32, ROWS, 2 * HEAD)
    pair = lax.all_to_all(pair, ("z", "y"), 0, 0, tiled=True)
    own = [pair] + [pull(pair, "x", s) for s in (1, 3, 2)]
    own[2], own[3] = own[3], own[2]
    other = [swap(t) for t in own]

    rows = jnp.concatenate(row_pieces, axis=0)
    weights = jnp.concatenate(weight_pieces, axis=0)
    weights_other = swap(weights)
    cos_q, sin_q = rotations(places.reshape(4 * ROWS))

    def project(w):
        q = lax.dot_general(w, rows, (((1,), (1,)), ((), ())), preferred_element_type=F32)
        q = q.reshape(4, 2, 32, 4 * ROWS)
        a, b = q[:, 0], q[:, 1]
        return jnp.concatenate([a * cos_q - b * sin_q, b * cos_q + a * sin_q], axis=1).astype(BF)

    q = ordered(project(weights), project(weights_other), c)
    q = lax.dynamic_slice_in_dim(jnp.concatenate([q, q], axis=1), (4 - x) % 4, 4, 1)
    q = jnp.transpose(q, (1, 0, 2, 3)).reshape(8, HEAD, 4 * ROWS)
    q = lax.all_to_all(q, "z", 0, 0, tiled=True)

    slot = jnp.arange(3, dtype=jnp.int32)
    meta = jnp.where(slot == 0, x, jnp.where(slot == 1, y, c))
    sink = lax.dynamic_slice_in_dim(sinks, 8 * y + z, 1, 0)
    out = attend(block_of, meta.astype(jnp.int32), sink, own, other, q)

    out = lax.all_to_all(out, ("z", "y"), 0, 0, tiled=True)
    out = out.reshape(8, 4, 32, 2, HEAD)
    return jnp.transpose(out, (3, 2, 1, 0, 4)).reshape(ROWS, 32 * HEAD)


def solution(mesh):
    fine = Mesh(mesh.devices.reshape(8, 4, 4, 2), ("z", "y", "x", "c"))
    whole = ("z", "y", "x", "c")

    return jax.shard_map(
        per_device,
        mesh=fine,
        in_specs=(P(whole, None), P(None, ("y", "x", "c")), P(), P(), P()),
        out_specs=P(whole, None),
        check_vma=False,
    )
```

```python
import jax
import jax.numpy as jnp
from jax import lax
from jax.experimental import pallas as pl
from jax.experimental.pallas import tpu as pltpu
from jax.sharding import Mesh, PartitionSpec as P


HEAD = 64
NBLK = 32
BLK = 512
ROWS = 64
GROUP = 4 * BLK
ROPE_BASE = 150000.0
NEG = -1e30
EXPC = 1.4426950408889634 / 8.0
BF = jnp.bfloat16
F32 = jnp.float32


def attend_kernel(
    inv_ref, meta_ref, sink_ref, k0, k1, k2, k3, o0, o1, o2, o3, q_ref, o_ref,
    kvs, vts, qs, bias, s_a, s_b, s_c, c_a, c_b, c_c,
):
    x_own = meta_ref[0]
    y_tile = meta_ref[1]
    core = meta_ref[2]
    off = (2 * x_own + core) * ROWS

    def prepare(s, _):
        b = inv_ref[s]
        for step, pair in enumerate(((k0, o0), (k1, o1), (k2, o2), (k3, o3))):
            for ref, at in zip(pair, (core, 1 - core)):
                place = 2 * lax.rem(x_own + step, 4) + at
                start = pl.multiple_of(s * BLK + place * ROWS, ROWS)
                kvs[pl.ds(start, ROWS), :] = ref[b]
        t = jnp.transpose(kvs[pl.ds(pl.multiple_of(s * BLK, BLK), BLK), :])
        vts[s, 0:HEAD, :] = t[HEAD : 2 * HEAD, :]
        vts[s, HEAD : HEAD + 16, :] = jnp.ones((16, BLK), BF)
        return 0

    lax.fori_loop(0, NBLK, prepare, 0, unroll=4)
    for k in range(8):
        rows = jnp.transpose(q_ref[k])
        wide = jnp.concatenate([rows, jnp.zeros((4 * ROWS, HEAD), BF)], axis=1)
        qs[k] = wide.reshape(4, ROWS, 2 * HEAD)

    col = lax.broadcasted_iota(jnp.int32, (1, 256), 1)
    limit = (col // ROWS) * BLK + lax.rem(col, ROWS) + off

    def mask_rows(u, _):
        start = pl.multiple_of(u * 256, 256)
        row = lax.broadcasted_iota(jnp.int32, (256, 256), 0) + start
        bias[pl.ds(start, 256), :] = jnp.where(row <= limit, 0.0, NEG)
        return 0

    lax.fori_loop(0, GROUP // 256, mask_rows, 0)

    def qtile(i):
        parts = []
        for j in range(4):
            b = inv_ref[i * 4 + j]
            parts.append(qs[b // 4, lax.rem(lax.rem(b, 4) - y_tile + 4, 4)])
        return jnp.concatenate(parts, axis=0)

    def qk(q, g, s_ref, c_ref, masked=False):
        top = None
        for u in range(4):
            start = pl.multiple_of(g * GROUP + u * BLK, BLK)
            scores = lax.dot_general(
                kvs[pl.ds(start, BLK), :], q, (((1,), (1,)), ((), ())), preferred_element_type=F32
            )
            if masked:
                scores = scores + bias[u * BLK : (u + 1) * BLK, :]
            s_ref[u * BLK : (u + 1) * BLK, :] = scores
            part = jnp.max(scores.reshape(BLK // 8, 8, 256), axis=0)
            top = part if top is None else jnp.maximum(top, part)
        c_ref[...] = top

    def soft(g, s_ref, c_ref, m, acc, masked=False):
        scores = s_ref[...]
        if masked:
            scores = scores + bias[...]
            top = jnp.max(scores.reshape(GROUP // 8, 8, 256), axis=0)
        else:
            top = c_ref[...]
        new = jnp.maximum(m, jnp.max(top, axis=0, keepdims=True))
        factor = jnp.exp2((m - new) * EXPC)
        weight = jnp.exp2((scores - new) * EXPC).astype(BF)
        values = jnp.concatenate([vts[g * 4 + u] for u in range(4)], axis=1)
        return new, acc * factor + jnp.dot(values, weight, preferred_element_type=F32)

    def finish(i, acc):
        done = jnp.transpose(acc[0:HEAD] / acc[HEAD : HEAD + 1]).astype(BF)
        for j in range(4):
            rows = done[j * ROWS : (j + 1) * ROWS]
            o_ref[inv_ref[i * 4 + j]] = jnp.concatenate([rows[0:32], rows[32:64]], axis=1)

    def two_tiles(i, _):
        a, b = 2 * i, 2 * i + 1
        q_a, q_b, q_next = qtile(a), qtile(b), qtile(jnp.minimum(a + 2, 6))
        m = jnp.full((1, 256), sink_ref[0] * 8.0, F32)
        acc = jnp.concatenate([jnp.zeros((HEAD, 256), F32), jnp.ones((16, 256), F32)], axis=0)

        def full(g, carry):
            m_a, acc_a, m_b, acc_b = carry
            qk(q_b, g, s_b, c_b)
            m_a, acc_a = soft(g, s_a, c_a, m_a, acc_a)
            qk(q_a, g + 1, s_a, c_a)
            m_b, acc_b = soft(g, s_b, c_b, m_b, acc_b)
            return m_a, acc_a, m_b, acc_b

        m_a, acc_a, m_b, acc_b = lax.fori_loop(0, a, full, (m, acc, m, acc))
        qk(q_b, a, s_b, c_b)
        m_a, acc_a = soft(a, s_a, c_a, m_a, acc_a, True)
        qk(q_b, b, s_c, c_c, True)
        m_b, acc_b = soft(a, s_b, c_b, m_b, acc_b)
        finish(a, acc_a)
        qk(q_next, 0, s_a, c_a)
        m_b, acc_b = soft(b, s_c, c_c, m_b, acc_b)
        finish(b, acc_b)
        return 0

    qk(qtile(0), 0, s_a, c_a)
    lax.fori_loop(0, 4, two_tiles, 0)


def attend(inv, meta, sink, own, other, q):
    return pl.pallas_call(
        attend_kernel,
        out_shape=jax.ShapeDtypeStruct((NBLK, 32, 128), BF),
        in_specs=[pl.BlockSpec(memory_space=pltpu.SMEM)] * 3
        + [pl.BlockSpec(memory_space=pltpu.VMEM)] * 9,
        out_specs=pl.BlockSpec(memory_space=pltpu.VMEM),
        scratch_shapes=[
            pltpu.VMEM((NBLK * BLK, 2 * HEAD), BF),
            pltpu.VMEM((NBLK, HEAD + 16, BLK), BF),
            pltpu.VMEM((8, 4, ROWS, 2 * HEAD), BF),
            pltpu.VMEM((GROUP, 256), F32),
        ]
        + [pltpu.VMEM((GROUP, 256), F32)] * 3
        + [pltpu.VMEM((8, 256), F32)] * 3,
        compiler_params=pltpu.CompilerParams(vmem_limit_bytes=50 * 2**20),
        name="attend",
    )(inv, meta, sink, *own, *other, q)


def project_kernel(
    meta_ref, cos_ref, sin_ref, r0, r1, r2, r3, w0, w1, w2, w3, v0, v1, v2, v3, q_ref, rows, weights
):
    x_own = meta_ref[0]
    core = meta_ref[2]
    width = r0.shape[1]
    edge = width // 128 * 128
    rows[:, edge:] = jnp.zeros((rows.shape[0], rows.shape[1] - edge), BF)
    weights[:, edge:] = jnp.zeros((weights.shape[0], weights.shape[1] - edge), BF)
    for s, ref in enumerate((r0, r1, r2, r3)):
        rows[s * ROWS : (s + 1) * ROWS, 0:width] = ref[...]
    for s, ref in enumerate((w0, w1, w2, w3, v0, v1, v2, v3)):
        weights[s * HEAD : (s + 1) * HEAD, 0:width] = ref[...]
    q = lax.dot_general(
        weights[...], rows[...], (((1,), (1,)), ((), ())), preferred_element_type=F32
    )
    cos, sin = cos_ref[...], sin_ref[...]
    for s in range(8):
        a = q[s * HEAD : s * HEAD + 32]
        b = q[s * HEAD + 32 : (s + 1) * HEAD]
        turned = jnp.concatenate([a * cos - b * sin, b * cos + a * sin], axis=0).astype(BF)
        side = core if s < 4 else 1 - core
        q_ref[2 * lax.rem(x_own + s % 4, 4) + side] = turned


def project(meta, cos, sin, rows, weights, others):
    return pl.pallas_call(
        project_kernel,
        out_shape=jax.ShapeDtypeStruct((8, HEAD, 4 * ROWS), BF),
        in_specs=[pl.BlockSpec(memory_space=pltpu.SMEM)]
        + [pl.BlockSpec(memory_space=pltpu.VMEM)] * 14,
        out_specs=pl.BlockSpec(memory_space=pltpu.VMEM),
        scratch_shapes=[pltpu.VMEM((4 * ROWS, 3072), BF), pltpu.VMEM((8 * HEAD, 3072), BF)],
        compiler_params=pltpu.CompilerParams(vmem_limit_bytes=32 * 2**20),
        name="project",
    )(meta, cos, sin, *rows, *weights, *others)


def pull(value, axis, shift):
    size = lax.axis_size(axis)
    return lax.ppermute(value, axis, [((i + shift) % size, i) for i in range(size)])


def swap(value):
    return lax.ppermute(value, "c", [(0, 1), (1, 0)])


def rotations(places):
    inverse = ROPE_BASE ** (-(jnp.arange(HEAD // 2, dtype=F32) * 2.0) / HEAD)
    angles = places.astype(F32)[None, :] * inverse[:, None]
    return jnp.cos(angles), jnp.sin(angles)


def per_device(tokens, query_weight, key_value_weight, block_places, sinks):
    z, y, x, c = (lax.axis_index(a) for a in "zyxc")
    weight_rows = query_weight.T
    row_pieces = [tokens] + [pull(tokens, "y", s) for s in (1, 2, 3)]
    weight_pieces = [weight_rows] + [pull(weight_rows, "x", s) for s in (1, 2, 3)]

    table = jnp.arange(NBLK, dtype=jnp.int32)
    block_of = jnp.sum(
        jnp.where(block_places[None, :] == table[:, None], table[None, :], 0), axis=1
    ).astype(jnp.int32)
    own_blocks = 4 * z + (y + jnp.arange(4, dtype=jnp.int32)) % 4
    own_places = jnp.sum(
        jnp.where(own_blocks[:, None] == table[None, :], block_places[None, :], 0), axis=1
    )
    places = (
        own_places[:, None] * BLK + (2 * x + c) * ROWS + jnp.arange(ROWS, dtype=jnp.int32)[None, :]
    )

    cos, sin = (t.T[:, None, :] for t in rotations(places[0]))
    kv = jnp.dot(tokens, key_value_weight, preferred_element_type=F32)
    keys = kv[:, :512].reshape(ROWS, 8, 2, 32)
    first, second = keys[:, :, 0], keys[:, :, 1]
    keys = jnp.concatenate([first * cos - second * sin, second * cos + first * sin], axis=-1)
    pair = jnp.concatenate([keys, kv[:, 512:].reshape(ROWS, 8, HEAD)], axis=-1).astype(BF)
    pair = jnp.transpose(pair.reshape(ROWS, 4, 2, 2 * HEAD), (2, 1, 0, 3))
    pair = jnp.broadcast_to(pair[:, None], (2, 4, 4, ROWS, 2 * HEAD)).reshape(32, ROWS, 2 * HEAD)
    pair = lax.all_to_all(pair, ("z", "y"), 0, 0, tiled=True)
    own = [pair] + [pull(pair, "x", s) for s in (1, 3, 2)]
    own[2], own[3] = own[3], own[2]
    other = [swap(t) for t in own]

    other_pieces = [swap(t) for t in weight_pieces]
    slot = jnp.arange(3, dtype=jnp.int32)
    meta = jnp.where(slot == 0, x, jnp.where(slot == 1, y, c)).astype(jnp.int32)
    cos_q, sin_q = rotations(places.reshape(4 * ROWS))
    q = project(meta, cos_q, sin_q, row_pieces, weight_pieces, other_pieces)
    q = lax.all_to_all(q, "z", 0, 0, tiled=True)

    sink = lax.dynamic_slice_in_dim(sinks, 8 * y + z, 1, 0)
    out = attend(block_of, meta, sink, own, other, q)

    out = lax.all_to_all(out, ("z", "y"), 0, 0, tiled=True)
    out = out.reshape(8, 4, 32, 2, HEAD)
    return jnp.transpose(out, (3, 2, 1, 0, 4)).reshape(ROWS, 32 * HEAD)


def solution(mesh):
    fine = Mesh(mesh.devices.reshape(8, 4, 4, 2), ("z", "y", "x", "c"))
    whole = ("z", "y", "x", "c")

    return jax.shard_map(
        per_device,
        mesh=fine,
        in_specs=(P(whole, None), P(None, ("y", "x", "c")), P(), P(), P()),
        out_specs=P(whole, None),
        check_vma=False,
    )
```

```python
import jax
import jax.numpy as jnp
from jax import lax
from jax.experimental import pallas as pl
from jax.experimental.pallas import tpu as pltpu
from jax.sharding import Mesh, PartitionSpec as P


HEAD = 64
NBLK = 32
BLK = 512
ROWS = 64
GROUP = 4 * BLK
ROPE_BASE = 150000.0
NEG = -1e30
EXPC = 1.4426950408889634 / 8.0
BF = jnp.bfloat16
F32 = jnp.float32


def attend_kernel(
    inv_ref, meta_ref, sink_ref, k0, k1, k2, k3, o0, o1, o2, o3, q_ref, o_ref,
    kvs, vts, qs, bias, s_a, s_b, c_a, c_b,
):
    x_own = meta_ref[0]
    y_tile = meta_ref[1]
    core = meta_ref[2]
    off = (2 * x_own + core) * ROWS

    def prepare(s, _):
        b = inv_ref[s]
        for step, pair in enumerate(((k0, o0), (k1, o1), (k2, o2), (k3, o3))):
            for ref, at in zip(pair, (core, 1 - core)):
                place = 2 * lax.rem(x_own + step, 4) + at
                start = pl.multiple_of(s * BLK + place * ROWS, ROWS)
                kvs[pl.ds(start, ROWS), :] = ref[lax.rem(b, 4) * 8 + b // 4]
        t = jnp.transpose(kvs[pl.ds(pl.multiple_of(s * BLK, BLK), BLK), :])
        vts[s, 0:HEAD, :] = t[HEAD : 2 * HEAD, :]
        vts[s, HEAD : HEAD + 16, :] = jnp.ones((16, BLK), BF)
        return 0

    lax.fori_loop(0, NBLK, prepare, 0, unroll=8)
    for k in range(8):
        rows = jnp.transpose(q_ref[k])
        wide = jnp.concatenate([rows, jnp.zeros((4 * ROWS, HEAD), BF)], axis=1)
        qs[k] = wide.reshape(4, ROWS, 2 * HEAD)

    col = lax.broadcasted_iota(jnp.int32, (1, 256), 1)
    limit = (col // ROWS) * BLK + lax.rem(col, ROWS) + off

    def mask_rows(u, _):
        start = pl.multiple_of(u * 256, 256)
        row = lax.broadcasted_iota(jnp.int32, (256, 256), 0) + start
        bias[pl.ds(start, 256), :] = jnp.where(row <= limit, 0.0, NEG)
        return 0

    lax.fori_loop(0, GROUP // 256, mask_rows, 0, unroll=2)

    def qtile(i):
        parts = []
        for j in range(4):
            b = inv_ref[i * 4 + j]
            parts.append(qs[b // 4, lax.rem(lax.rem(b, 4) - y_tile + 4, 4)])
        return jnp.concatenate(parts, axis=0)

    def qk(q, g, s_ref, c_ref, masked=False):
        top = None
        for u in range(4):
            start = pl.multiple_of(g * GROUP + u * BLK, BLK)
            scores = lax.dot_general(
                kvs[pl.ds(start, BLK), :], q, (((1,), (1,)), ((), ())), preferred_element_type=F32
            )
            if masked:
                scores = scores + bias[u * BLK : (u + 1) * BLK, :]
            s_ref[u * BLK : (u + 1) * BLK, :] = scores
            part = jnp.max(scores.reshape(BLK // 8, 8, 256), axis=0)
            top = part if top is None else jnp.maximum(top, part)
        c_ref[...] = top

    def soft(g, s_ref, c_ref, m, acc, masked=False):
        scores = s_ref[...]
        if masked:
            scores = scores + bias[...]
            top = jnp.max(scores.reshape(GROUP // 8, 8, 256), axis=0)
        else:
            top = c_ref[...]
        new = jnp.maximum(m, jnp.max(top, axis=0, keepdims=True))
        factor = jnp.exp2((m - new) * EXPC)
        weight = jnp.exp2((scores - new) * EXPC).astype(BF)
        values = jnp.concatenate([vts[g * 4 + u] for u in range(4)], axis=1)
        return new, acc * factor + jnp.dot(values, weight, preferred_element_type=F32)

    def finish(i, acc):
        done = jnp.transpose(acc[0:HEAD] / acc[HEAD : HEAD + 1]).astype(BF)
        for j in range(4):
            rows = done[j * ROWS : (j + 1) * ROWS]
            b = inv_ref[i * 4 + j]
            o_ref[lax.rem(b, 4) * 8 + b // 4] = jnp.concatenate([rows[0:32], rows[32:64]], axis=1)

    s_refs, c_refs = (s_a, s_b), (c_a, c_b)
    units = [(t, g) for g in range(4) for t in range(g, 4)]

    def four_tiles(i, _):
        base = 4 * i
        tiles = [qtile(base + t) for t in range(4)]
        q_next = qtile(jnp.minimum(base + 4, 4))
        m = jnp.full((1, 256), sink_ref[0] * 8.0, F32)
        acc = jnp.concatenate([jnp.zeros((HEAD, 256), F32), jnp.ones((16, 256), F32)], axis=0)

        def full(g, carry):
            ms, accs = list(carry[:4]), list(carry[4:])
            for t in range(4):
                if t < 3:
                    qk(tiles[t + 1], g, s_refs[(t + 1) % 2], c_refs[(t + 1) % 2])
                else:
                    qk(tiles[0], g + 1, s_a, c_a)
                ms[t], accs[t] = soft(g, s_refs[t % 2], c_refs[t % 2], ms[t], accs[t])
            return (*ms, *accs)

        carry = lax.fori_loop(0, base, full, (m,) * 4 + (acc,) * 4)
        ms, accs = list(carry[:4]), list(carry[4:])
        for k, (t, g) in enumerate(units):
            if k + 1 < len(units):
                t2, g2 = units[k + 1]
                qk(tiles[t2], base + g2, s_refs[(k + 1) % 2], c_refs[(k + 1) % 2], t2 == g2)
            else:
                qk(q_next, 0, s_a, c_a)
            ms[t], accs[t] = soft(
                base + g, s_refs[k % 2], c_refs[k % 2], ms[t], accs[t], k == 0
            )
            if t == g:
                finish(base + t, accs[t])
        return 0

    qk(qtile(0), 0, s_a, c_a)
    lax.fori_loop(0, 2, four_tiles, 0)


def attend(inv, meta, sink, own, other, q):
    return pl.pallas_call(
        attend_kernel,
        out_shape=jax.ShapeDtypeStruct((NBLK, 32, 128), BF),
        in_specs=[pl.BlockSpec(memory_space=pltpu.SMEM)] * 3
        + [pl.BlockSpec(memory_space=pltpu.VMEM)] * 9,
        out_specs=pl.BlockSpec(memory_space=pltpu.VMEM),
        scratch_shapes=[
            pltpu.VMEM((NBLK * BLK, 2 * HEAD), BF),
            pltpu.VMEM((NBLK, HEAD + 16, BLK), BF),
            pltpu.VMEM((8, 4, ROWS, 2 * HEAD), BF),
            pltpu.VMEM((GROUP, 256), F32),
        ]
        + [pltpu.VMEM((GROUP, 256), F32)] * 2
        + [pltpu.VMEM((8, 256), F32)] * 2,
        compiler_params=pltpu.CompilerParams(vmem_limit_bytes=50 * 2**20),
        name="attend",
    )(inv, meta, sink, *own, *other, q)


def project_kernel(
    meta_ref, cos_ref, sin_ref, r0, r1, r2, r3, w0, w1, w2, w3, v0, v1, v2, v3, q_ref, rows, weights
):
    x_own = meta_ref[0]
    core = meta_ref[2]
    width = r0.shape[1]
    edge = width // 128 * 128
    rows[:, edge:] = jnp.zeros((rows.shape[0], rows.shape[1] - edge), BF)
    weights[:, edge:] = jnp.zeros((weights.shape[0], weights.shape[1] - edge), BF)
    for s, ref in enumerate((r0, r1, r2, r3)):
        rows[s * ROWS : (s + 1) * ROWS, 0:width] = ref[...]
    for s, ref in enumerate((w0, w1, w2, w3, v0, v1, v2, v3)):
        weights[s * HEAD : (s + 1) * HEAD, 0:width] = ref[...]
    q = lax.dot_general(
        weights[...], rows[...], (((1,), (1,)), ((), ())), preferred_element_type=F32
    )
    cos, sin = cos_ref[...], sin_ref[...]
    for s in range(8):
        a = q[s * HEAD : s * HEAD + 32]
        b = q[s * HEAD + 32 : (s + 1) * HEAD]
        turned = jnp.concatenate([a * cos - b * sin, b * cos + a * sin], axis=0).astype(BF)
        side = core if s < 4 else 1 - core
        q_ref[2 * lax.rem(x_own + s % 4, 4) + side] = turned


def project(meta, cos, sin, rows, weights, others):
    return pl.pallas_call(
        project_kernel,
        out_shape=jax.ShapeDtypeStruct((8, HEAD, 4 * ROWS), BF),
        in_specs=[pl.BlockSpec(memory_space=pltpu.SMEM)]
        + [pl.BlockSpec(memory_space=pltpu.VMEM)] * 14,
        out_specs=pl.BlockSpec(memory_space=pltpu.VMEM),
        scratch_shapes=[pltpu.VMEM((4 * ROWS, 3072), BF), pltpu.VMEM((8 * HEAD, 3072), BF)],
        compiler_params=pltpu.CompilerParams(vmem_limit_bytes=32 * 2**20),
        name="project",
    )(meta, cos, sin, *rows, *weights, *others)


def pull(value, axis, shift):
    size = lax.axis_size(axis)
    return lax.ppermute(value, axis, [((i + shift) % size, i) for i in range(size)])


def swap(value):
    return lax.ppermute(value, "c", [(0, 1), (1, 0)])


def rotations(places):
    inverse = ROPE_BASE ** (-(jnp.arange(HEAD // 2, dtype=F32) * 2.0) / HEAD)
    angles = places.astype(F32)[None, :] * inverse[:, None]
    return jnp.cos(angles), jnp.sin(angles)


def per_device(tokens, query_weight, key_value_weight, block_places, sinks):
    z, y, x, c = (lax.axis_index(a) for a in "zyxc")
    weight_rows = query_weight.T
    row_pieces = [tokens] + [pull(tokens, "y", s) for s in (1, 2, 3)]
    weight_pieces = [weight_rows] + [pull(weight_rows, "x", s) for s in (1, 2, 3)]

    table = jnp.arange(NBLK, dtype=jnp.int32)
    block_of = jnp.sum(
        jnp.where(block_places[None, :] == table[:, None], table[None, :], 0), axis=1
    ).astype(jnp.int32)
    own_blocks = 4 * z + (y + jnp.arange(4, dtype=jnp.int32)) % 4
    own_places = jnp.sum(
        jnp.where(own_blocks[:, None] == table[None, :], block_places[None, :], 0), axis=1
    )
    places = (
        own_places[:, None] * BLK + (2 * x + c) * ROWS + jnp.arange(ROWS, dtype=jnp.int32)[None, :]
    )

    cos, sin = (t.T[:, None, :] for t in rotations(places[0]))
    kv = jnp.dot(tokens, key_value_weight, preferred_element_type=F32)
    keys = kv[:, :512].reshape(ROWS, 8, 2, 32)
    first, second = keys[:, :, 0], keys[:, :, 1]
    keys = jnp.concatenate([first * cos - second * sin, second * cos + first * sin], axis=-1)
    pair = jnp.concatenate([keys, kv[:, 512:].reshape(ROWS, 8, HEAD)], axis=-1).astype(BF)
    pair = jnp.transpose(pair, (1, 0, 2))
    pair = jnp.broadcast_to(pair[:, None], (8, 4, ROWS, 2 * HEAD)).reshape(32, ROWS, 2 * HEAD)
    pair = lax.all_to_all(pair, ("y", "z"), 0, 0, tiled=True)
    own = [pair] + [pull(pair, "x", s) for s in (1, 3, 2)]
    own[2], own[3] = own[3], own[2]
    other = [swap(t) for t in own]

    other_pieces = [swap(t) for t in weight_pieces]
    slot = jnp.arange(3, dtype=jnp.int32)
    meta = jnp.where(slot == 0, x, jnp.where(slot == 1, y, c)).astype(jnp.int32)
    cos_q, sin_q = rotations(places.reshape(4 * ROWS))
    q = project(meta, cos_q, sin_q, row_pieces, weight_pieces, other_pieces)
    q = lax.all_to_all(q, "z", 0, 0, tiled=True)

    sink = lax.dynamic_slice_in_dim(sinks, 8 * y + z, 1, 0)
    out = attend(block_of, meta, sink, own, other, q)

    out = lax.all_to_all(out, ("y", "z"), 0, 0, tiled=True)
    out = out.reshape(32, 32, 2, HEAD)
    return jnp.transpose(out, (2, 1, 0, 3)).reshape(ROWS, 32 * HEAD)


def solution(mesh):
    fine = Mesh(mesh.devices.reshape(8, 4, 4, 2), ("z", "y", "x", "c"))
    whole = ("z", "y", "x", "c")

    return jax.shard_map(
        per_device,
        mesh=fine,
        in_specs=(P(whole, None), P(None, ("y", "x", "c")), P(), P(), P()),
        out_specs=P(whole, None),
        check_vma=False,
    )
```
